32 devices in a mesh: groups: 2 (over x), bay: 16 (over z, y, core).
Axes of the slice: x: 2, y: 2, z: 4, core: 2. Of those that a mesh axis runs over, the one named last changes fastest.
Arguments:
- traces: bfloat16 [16, 512, 2048], P('bay', 'groups'), parts along dimension 1, may hold values from -6 to 6
- operator: bfloat16 [16, 2048, 2048], P('bay'), may hold values from -0.09375 to 0.09375
- loads: bfloat16 [16, 16, 2048], P('bay'), may hold values from -6 to 6
- seeds: int32 [512], P('groups'), parts along dimension 0, may hold values from 0 to 99999
- patches: int32 [16, 512], P('bay', 'groups'), parts along dimension 1, may hold values from 0 to 15
- trace_map: int32 [16, 1024], P('bay'), may hold values from 0 to 1023, each once within a row
Outputs:
- final_traces: bfloat16 [16, 512, 2048], P('bay', 'groups'), parts along dimension 1
The draws below stay inside these ranges and needn't reach their ends.
There are 2 independent parts, one for each index of `groups`. The reference program is written for one: setup_inputs(seed, part) draws one part's arguments, and reference() takes and returns one part's arrays. A program takes and returns all parts, laid end to end along the dimension named above; an argument that names none is the same for every part. Nothing has to cross between parts.
Inputs may be any that keep to these rules, and one draw needn't show every extreme that they name: `trace_map`: each row is a permutation of 0 to 1023.
All inputs are finite; a program needn't handle non-finite values.
Results may differ from the reference program's by a relative error of at most 0.0065.
Values may be sent and summed in bfloat16 or wider, within the bound.
A program may use at most 64 MiB of HBM per device.

```python
import jax
import jax.numpy as jnp
from jax import lax

TRACES = 2048
ONWARD = 1024
LATERAL = 512
CASES = 256
TICKS = 6
STRIPS = 4
PATCHES = 16
N_BAY = 16


def plant(drawn, rng, least, largest):
    dims = drawn.shape
    index_at = [jax.random.randint(jax.random.fold_in(rng, axis), (), 0, dims[axis]) for axis in range(len(dims))]
    drawn = drawn.at[tuple(index_at)].set(least)
    longest = dims.index(max(dims))
    index_at[longest] = (index_at[longest] + 1) % dims[longest]
    return drawn.at[tuple(index_at)].set(largest)


def block_levels(own_key, extent, pieces, least, high):
    level, own = 1.0, jax.random.fold_in(own_key, 6)
    for dim, shards_of in pieces:
        steps = jnp.exp(jax.random.uniform(jax.random.fold_in(own, dim), (shards_of,), jnp.float32, least / len(pieces), high / len(pieces)))
        level = level * jnp.repeat(steps, extent[dim] // shards_of).reshape([-1 if axis == dim else 1 for axis in range(len(extent))])
    return level


def normal_values(stream_key, shape, scale, reach, shards=(), kind=jnp.bfloat16):
    entries = scale * jax.random.normal(stream_key, shape, jnp.float32)
    if shards:
        entries = entries * block_levels(stream_key, shape, shards, -0.22, 0.18)
    return jnp.clip(entries, -reach, reach).astype(kind)


def setup_inputs(seed: int = 0, part: int = 0) -> dict:
    splits = jax.random.split(jax.random.key(seed), 7)
    part_splits = jax.random.split(jax.random.fold_in(splits[6], part), 7)
    traces = normal_values(part_splits[0], (N_BAY, CASES, TRACES), 1.0, 6.0, ((0, 16),))
    operator = normal_values(splits[1], (N_BAY, TRACES, TRACES), (2 * TRACES) ** -0.5, 0.09375, ((0, 16),))
    loads = normal_values(splits[2], (N_BAY, PATCHES, TRACES), 1.0, 6.0, ((0, 16),))
    seeds = plant(jax.random.randint(part_splits[3], (CASES,), 0, 100000), jax.random.fold_in(part_splits[3], 1), 0, 99999).astype(jnp.int32)
    patches = plant(jax.random.randint(part_splits[4], (N_BAY, CASES), 0, PATCHES), jax.random.fold_in(part_splits[4], 1), 0, PATCHES - 1).astype(jnp.int32)
    trace_map = jax.vmap(lambda own: jax.random.permutation(own, ONWARD))(jax.random.split(splits[5], N_BAY)).reshape((N_BAY, ONWARD)).astype(jnp.int32)
    return {"traces": traces, "operator": operator, "loads": loads, "seeds": seeds, "patches": patches, "trace_map": trace_map}


def reference(traces, operator, loads, seeds, patches, trace_map):
    index = jnp.arange(N_BAY, dtype=jnp.int32)
    near_ids = jnp.bitwise_xor(index, 1)
    far_ids = jnp.bitwise_xor(index, 2)
    patch_rows = jax.vmap(lambda table, picks: jnp.take(table, picks, axis=0))(loads, patches).astype(jnp.float32)
    state = traces
    for tick in range(TICKS):
        amplitude = (((seeds * 7 + 13 * tick) % 97) - 48).astype(jnp.float32) / 32.0
        source = amplitude[None, :, None] * patch_rows
        onward = state[:, :, :ONWARD]
        shifted = jnp.concatenate([jnp.zeros((STRIPS, CASES, ONWARD), jnp.bfloat16), onward[:N_BAY - STRIPS]], axis=0)
        mapped = jax.vmap(lambda block, order: jnp.take(block, order, axis=1))(shifted, trace_map)
        near = state[near_ids][:, :, ONWARD:ONWARD + LATERAL]
        far = state[far_ids][:, :, ONWARD + LATERAL:]
        incoming = jnp.concatenate([mapped, near, far], axis=2)
        product = lax.map(lambda pair: jnp.dot(pair[0], pair[1], preferred_element_type=jnp.float32), (incoming, operator))
        state = (product + source).astype(jnp.bfloat16)
    return state
```

```python
import functools

import jax
import jax.numpy as jnp
from jax import lax
from jax.experimental import pallas as pl
from jax.experimental.pallas import tpu as pltpu
from jax.sharding import PartitionSpec as P

TICKS = 6
STRIPS = 4
CHUNKS = 2
PIECES = 4
PERIOD = 97
LANES = 512
MESH = pl.DeviceIdType.MESH


def dot(a, b):
    return jnp.dot(a, b, preferred_element_type=jnp.float32)


def kernel(
    count, traces, operator, loads, seeds, patches, trace_map, out,
    weights, mapped, one_hot, state_on, state_side, got_on, got_side,
    total, table, seed_row, pick_row, map_row, picked,
    in_sem, weight_sem, trace_sem, send_sem, on_sem, side_sem,
):
    me = lax.axis_index("bay")
    rows, size = state_on.shape[2:]
    lateral = state_side.shape[3]
    onward = PIECES * size
    width = onward + 2 * lateral
    part = rows // CHUNKS
    has_next = me + STRIPS < count
    has_prev = me >= STRIPS
    near = me + 1 - 2 * (me % 2)
    far = me + 2 - 4 * ((me // 2) % 2)
    targets = (me + STRIPS,) * PIECES + (near, far)
    starts = tuple(q * size for q in range(PIECES)) + (onward, onward + lateral)
    sizes = (size,) * PIECES + (lateral, lateral)
    sides = (PIECES, PIECES + 1)

    def rows_of(c):
        return pl.ds(c * part, part)

    def held(t, c, k):
        if k < PIECES:
            return state_on.at[t, k, rows_of(c)]
        return state_side.at[t, k - PIECES, rows_of(c)]

    def got(t, c, k):
        if k < PIECES:
            return got_on.at[t, k, rows_of(c)]
        return got_side.at[t, k - PIECES, rows_of(c)]

    small = [
        pltpu.make_async_copy(src, dst, in_sem.at[i])
        for i, (src, dst) in enumerate(
            ((trace_map, map_row), (seeds, seed_row), (patches, pick_row), (loads.at[0], table))
        )
    ]
    first = [
        [
            pltpu.make_async_copy(
                traces.at[0, rows_of(c), pl.ds(starts[k], sizes[k])], held(0, c, k), trace_sem.at[c, k // PIECES]
            )
            for k in range(PIECES + 2)
        ]
        for c in range(CHUNKS)
    ]
    halves = [
        pltpu.make_async_copy(
            operator.at[0, pl.ds(h * onward, onward)], weights.at[pl.ds(h * onward, onward)], weight_sem.at[h]
        )
        for h in range(2)
    ]
    for copy in first[0]:
        copy.start()

    barrier = pltpu.get_barrier_semaphore()

    def greet(device):
        pl.semaphore_signal(barrier, inc=1, device_id={"bay": device}, device_id_type=MESH)

    greet(near)
    greet(far)

    @pl.when(has_prev)
    def _():
        greet(me - STRIPS)

    for copy in small:
        copy.start()
    for c in range(1, CHUNKS):
        for copy in first[c]:
            copy.start()

    pl.semaphore_wait(barrier, 2 + has_next.astype(jnp.int32))

    last = TICKS - 1

    def signal_of(t, c, k):
        if k >= PIECES:
            return side_sem.at[t % 2, c]
        alone = k * ((t + 1) // TICKS) if c == CHUNKS - 1 else 0
        return on_sem.at[t * CHUNKS + c + alone]

    def copy_to(device, src, dst, kind, signal):
        return pltpu.make_async_remote_copy(
            src_ref=src,
            dst_ref=dst,
            send_sem=send_sem.at[kind],
            recv_sem=signal,
            device_id={"bay": device},
            device_id_type=MESH,
        )

    def remote(t, c, k):
        return copy_to(targets[k], held(t, c, k), got(t, c, k), k // PIECES, signal_of(t, c, k))

    def all_onward(t, c):
        here = (t, slice(None), rows_of(c))
        return copy_to(targets[0], state_on.at[here], got_on.at[here], 0, signal_of(t, c, 0))

    def both_sides(t, c):
        here = (t, slice(None), rows_of(c))
        return copy_to(near, state_side.at[here], got_side.at[here], 1, signal_of(t, c, PIECES))

    def send_onward(t, c, pieces):
        @pl.when(has_next)
        def _():
            for k in pieces:
                remote(t, c, k).start()

    def loaded(c, buffer, kind):
        dst = buffer.at[0, :, rows_of(c)]
        pltpu.make_async_copy(dst, dst, trace_sem.at[c, kind]).wait()

    every = tuple(range(PIECES))
    for c in range(CHUNKS):
        loaded(c, state_on, 0)
        send_onward(0, c, every)
        loaded(c, state_side, 1)
        for k in sides:
            remote(0, c, k).start()
        if c == 0:
            for copy in halves:
                copy.start()

    @pl.when(jnp.logical_not(has_prev))
    def _():
        got_on[...] = jnp.zeros_like(got_on)

    for copy in small:
        copy.wait()
    place = lax.broadcasted_iota(jnp.int32, one_hot.shape, 0)
    one_hot[...] = jnp.where(place == map_row[...], 1.0, 0.0).astype(jnp.bfloat16)
    value = seed_row[...] * 7
    guess = (value.astype(jnp.float32) * (1.0 / PERIOD)).astype(jnp.int32)
    rest = value - guess * PERIOD
    rest = jnp.where(rest < 0, rest + PERIOD, rest)
    rest = jnp.where(rest >= PERIOD, rest - PERIOD, rest)
    chosen = lax.broadcasted_iota(jnp.int32, picked.shape[1:], 0) == pick_row[...]
    for t in range(TICKS):
        turn = rest + (13 * t) % PERIOD
        turn = jnp.where(turn >= PERIOD, turn - PERIOD, turn)
        amplitude = (turn - 48).astype(jnp.float32) / 32.0
        picked[t] = jnp.where(chosen, amplitude, 0.0).astype(jnp.bfloat16)

    halves[0].wait()

    @pl.loop(0, width // LANES)
    def _(n):
        at = pl.ds(pl.multiple_of(n * LANES, LANES), LANES)
        for m in range(0, onward, 256):
            mapped[m : m + 256, at] = dot(one_hot[m : m + 256, :], weights[:onward, at]).astype(jnp.bfloat16)

    halves[1].wait()

    def sideways(t, c):
        here = rows_of(c)
        both_sides(t, c).wait_recv()

        @pl.loop(0, width // LANES)
        def _(n):
            at = pl.ds(pl.multiple_of(n * LANES, LANES), LANES)
            source = lax.dot_general(
                picked[t, :, here], table[:, at], (((0,), (0,)), ((), ())), preferred_element_type=jnp.float32
            )
            total[here, at] = (
                source
                + dot(got_side[t, 0, here], weights[onward : onward + lateral, at])
                + dot(got_side[t, 1, here], weights[onward + lateral :, at])
            )

    def arrive(t, c, pieces):
        @pl.when(has_prev)
        def _():
            if pieces == every:
                all_onward(t, c).wait_recv()
            else:
                for k in pieces:
                    remote(t, c, k).wait_recv()

    def block(t, c, column, pieces):
        here = rows_of(c)
        at = pl.ds(column, LANES)
        incoming = jnp.concatenate([got_on[t, q, here] for q in pieces], axis=1)
        return total[here, at] + dot(incoming, mapped[pieces[0] * size : (pieces[-1] + 1) * size, at])

    @pl.loop(0, TICKS - 1)
    def _(t):
        for c in range(CHUNKS):
            here = rows_of(c)
            sideways(t, c)
            arrive(t, c, every)
            for column in range(0, onward, LANES):
                value = block(t, c, column, every).astype(jnp.bfloat16)
                pieces = tuple(range(column // size, (column + LANES) // size))
                for q in pieces:
                    state_on[t + 1, q, here] = value[:, q * size - column : (q + 1) * size - column]
                send_onward(t + 1, c, pieces)
            for k in sides:
                for column in range(0, lateral, LANES):
                    value = block(t, c, starts[k] + column, every).astype(jnp.bfloat16)
                    state_side[t + 1, k - PIECES, here, column : column + LANES] = value
                remote(t + 1, c, k).start()

    columns = range(0, width, LANES)
    for c in range(CHUNKS):
        here = rows_of(c)
        sideways(last, c)
        rounds = (every,) if c < CHUNKS - 1 else tuple((q,) for q in every)
        for pieces in rounds[:-1]:
            arrive(last, c, pieces)
            for column in columns:
                total[here, column : column + LANES] = block(last, c, column, pieces)
        arrive(last, c, rounds[-1])
        for column in columns:
            out[0, here, column : column + LANES] = block(last, c, column, rounds[-1]).astype(jnp.bfloat16)

    copy_to(near, state_side, got_side, 1, side_sem.at[0, 0]).wait_send()

    @pl.when(has_next)
    def _():
        copy_to(targets[0], state_on, got_on, 0, on_sem.at[0]).wait_send()


def on_device(count, traces, operator, loads, seeds, patches, trace_map):
    _, rows, width = traces.shape
    onward = trace_map.shape[1]
    lateral = (width - onward) // 2
    depth = loads.shape[1]
    bf16, i32 = jnp.bfloat16, jnp.int32
    anywhere = pl.BlockSpec(memory_space=pl.ANY)
    dma = pltpu.SemaphoreType.DMA
    slots = (
        pltpu.VMEM((TICKS, PIECES, rows, onward // PIECES), bf16),
        pltpu.VMEM((TICKS, 2, rows, lateral), bf16),
    )
    return pl.pallas_call(
        functools.partial(kernel, count),
        name="sweep",
        out_shape=pltpu.VMEM(traces.shape, bf16),
        in_specs=[anywhere] * 6,
        out_specs=pl.BlockSpec(memory_space=pltpu.VMEM),
        scratch_shapes=[
            pltpu.VMEM((width, width), bf16),
            pltpu.VMEM((onward, width), bf16),
            pltpu.VMEM((onward, onward), bf16),
            *slots,
            *slots,
            pltpu.VMEM((rows, width), jnp.float32),
            pltpu.VMEM((depth, width), bf16),
            pltpu.VMEM((1, rows), i32),
            pltpu.VMEM((1, rows), i32),
            pltpu.VMEM((1, onward), i32),
            pltpu.VMEM((TICKS, depth, rows), bf16),
            dma((4,)),
            dma((2,)),
            dma((CHUNKS, 2)),
            dma((2,)),
            dma((TICKS * CHUNKS + PIECES - 1,)),
            dma((2, CHUNKS)),
        ],
        compiler_params=pltpu.CompilerParams(
            collective_id=0, has_side_effects=True, vmem_limit_bytes=60 * 2**20
        ),
    )(traces, operator, loads, seeds.reshape(1, rows), patches, trace_map)


def solution(mesh):
    placed = (
        P("bay", "groups", None),
        P("bay", None, None),
        P("bay", None, None),
        P("groups"),
        P("bay", "groups"),
        P("bay", None),
    )
    return jax.shard_map(
        functools.partial(on_device, mesh.shape["bay"]),
        mesh=mesh,
        in_specs=placed,
        out_specs=P("bay", "groups", None),
        check_vma=False,
    )
```

```python
import functools

import jax
import jax.numpy as jnp
from jax import lax
from jax.experimental import pallas as pl
from jax.experimental.pallas import tpu as pltpu
from jax.sharding import PartitionSpec as P

TICKS = 6
STRIPS = 4
CHUNKS = 2
PIECES = 4
ROUNDS = ((0, 1), (2,), (3,))
DEFER = 3
PERIOD = 97
LANES = 512
MESH = pl.DeviceIdType.MESH


def dot(a, b):
    return jnp.dot(a, b, preferred_element_type=jnp.float32)


def kernel(
    count, traces, operator, loads, seeds, patches, trace_map, early, total, mapped, tail,
    weights, one_hot, state_on, state_side, got_on, got_side,
    small, picked,
    in_sem, send_sem, on_sem, side_sem,
):
    me = lax.axis_index("bay")
    rows, size = state_on.shape[2:]
    lateral = state_side.shape[3]
    onward = PIECES * size
    width = onward + 2 * lateral
    depth = loads.shape[1]
    part = rows // CHUNKS
    has_next = me + STRIPS < count
    has_prev = me >= STRIPS
    near = me + 1 - 2 * (me % 2)
    far = me + 2 - 4 * ((me // 2) % 2)
    barrier = pltpu.get_barrier_semaphore()

    def greet(device):
        pl.semaphore_signal(barrier, inc=1, device_id={"bay": device}, device_id_type=MESH)

    @pl.when(has_prev)
    def _():
        greet(me - STRIPS)

    greet(far)
    greet(near)

    starts = tuple(q * size for q in range(PIECES)) + (onward, onward + lateral)
    sizes = (size,) * PIECES + (lateral, lateral)
    sides = (PIECES, PIECES + 1)

    def rows_of(c):
        return pl.ds(c * part, part)

    def span(pieces):
        return pl.ds(pieces[0], len(pieces))

    def held(t, c, k):
        if k < PIECES:
            return state_on.at[t, k, rows_of(c)]
        return state_side.at[t, k - PIECES, rows_of(c)]

    first = [
        pltpu.make_async_copy(
            traces.at[0, rows_of(c), pl.ds(starts[k], sizes[k])], held(0, c, k), in_sem.at[k // PIECES]
        )
        for c in range(CHUNKS)
        for k in range(PIECES + 2)
    ]
    lists = [
        pltpu.make_async_copy(src, small.at[:, pl.ds(begin, src.shape[1])], in_sem.at[2])
        for src, begin in ((trace_map, 0), (seeds, onward), (patches, onward + rows))
    ]
    upper = pltpu.make_async_copy(operator.at[0, pl.ds(0, onward)], weights.at[pl.ds(0, onward)], in_sem.at[0])
    lower = [
        pltpu.make_async_copy(operator.at[0, pl.ds(onward, onward)], weights.at[pl.ds(onward, onward)], in_sem.at[1]),
        pltpu.make_async_copy(loads.at[0], weights.at[pl.ds(width, depth)], in_sem.at[1]),
    ]
    for copy in first + lists:
        copy.start()

    pl.semaphore_wait(barrier, 2 + has_next.astype(jnp.int32))

    last = TICKS - 1

    def copy_to(device, src, dst, kind, signal):
        return pltpu.make_async_remote_copy(
            src_ref=src,
            dst_ref=dst,
            send_sem=send_sem.at[kind],
            recv_sem=signal,
            device_id={"bay": device},
            device_id_type=MESH,
        )

    def to_next(t, c, pieces):
        alone = 0
        if c == CHUNKS - 1 and pieces in ROUNDS:
            alone = ROUNDS.index(pieces) * ((t + 1) // TICKS)
        here = (t, span(pieces), rows_of(c))
        return copy_to(me + STRIPS, state_on.at[here], got_on.at[here], 0, on_sem.at[t * CHUNKS + c + alone])

    def to_side(t, c, k):
        here = (t, k - PIECES, rows_of(c))
        return copy_to((near, far)[k - PIECES], state_side.at[here], got_side.at[here], 1, side_sem.at[t % 2, c])

    def both_sides(t, c):
        here = (t, slice(None), rows_of(c))
        return copy_to(near, state_side.at[here], got_side.at[here], 1, side_sem.at[t % 2, c])

    def send_onward(t, c, groups):
        @pl.when(has_next)
        def _():
            for pieces in groups:
                to_next(t, c, pieces).start()

    def loaded(ref, which):
        pltpu.make_async_copy(ref, ref, in_sem.at[which]).wait()

    every = tuple(range(PIECES))
    deferred = jnp.logical_not(has_prev) & (me % 2 == 1)

    def send_first(c, when):
        @pl.when(has_next & when)
        def _():
            to_next(0, c, every).start()

    loaded(state_on.at[0], 0)
    send_first(0, True)
    for c in range(1, CHUNKS):
        send_first(c, jnp.logical_not(deferred))
    loaded(state_side.at[0], 1)
    for c in range(CHUNKS):
        for k in sides:
            to_side(0, c, k).start()
    for copy in [upper] + lower:
        copy.start()

    @pl.when(jnp.logical_not(has_prev))
    def _():
        got_on[...] = jnp.zeros_like(got_on)

    loaded(small, 2)
    map_row = small[:, :onward]
    seed_row = small[:, onward : onward + rows]
    pick_row = small[:, onward + rows :]
    place = lax.broadcasted_iota(jnp.int32, one_hot.shape, 0)
    one_hot[...] = jnp.where(place == map_row, 1.0, 0.0).astype(jnp.bfloat16)
    value = seed_row * 7
    guess = (value.astype(jnp.float32) * (1.0 / PERIOD)).astype(jnp.int32)
    rest = value - guess * PERIOD
    rest = jnp.where(rest < 0, rest + PERIOD, rest)
    rest = jnp.where(rest >= PERIOD, rest - PERIOD, rest)
    chosen = lax.broadcasted_iota(jnp.int32, picked.shape[1:], 0) == pick_row
    for t in range(TICKS):
        turn = rest + (13 * t) % PERIOD
        turn = jnp.where(turn >= PERIOD, turn - PERIOD, turn)
        amplitude = (turn - 48).astype(jnp.float32) / 32.0
        picked[t] = jnp.where(chosen, amplitude, 0.0).astype(jnp.bfloat16)

    upper.wait()

    @pl.loop(0, width // LANES)
    def _(n):
        at = pl.ds(pl.multiple_of(n * LANES, LANES), LANES)
        for m in range(0, onward, 256):
            mapped[m : m + 256, at] = dot(one_hot[m : m + 256, :], weights[:onward, at]).astype(jnp.bfloat16)

        for c in range(1, CHUNKS):
            send_first(c, deferred & (n == DEFER))

    loaded(weights.at[pl.ds(onward, onward + depth)], 1)

    def sideways(t, c):
        here = rows_of(c)
        both_sides(t, c).wait_recv()

        @pl.loop(0, width // LANES)
        def _(n):
            at = pl.ds(pl.multiple_of(n * LANES, LANES), LANES)
            source = lax.dot_general(
                picked[t, :, here], weights[width:, at], (((0,), (0,)), ((), ())), preferred_element_type=jnp.float32
            )
            total[here, at] = (
                source
                + dot(got_side[t, 0, here], weights[onward : onward + lateral, at])
                + dot(got_side[t, 1, here], weights[onward + lateral : width, at])
            )

    def arrive(t, c, pieces):
        @pl.when(has_prev)
        def _():
            to_next(t, c, pieces).wait_recv()

    def block(t, c, column, pieces):
        here = rows_of(c)
        at = pl.ds(column, LANES)
        incoming = jnp.concatenate([got_on[t, q, here] for q in pieces], axis=1)
        return total[here, at] + dot(incoming, mapped[pieces[0] * size : (pieces[-1] + 1) * size, at])

    @pl.loop(0, TICKS - 1)
    def _(t):
        for c in range(CHUNKS):
            here = rows_of(c)
            sideways(t, c)
            arrive(t, c, every)
            for column in range(0, onward, LANES):
                value = block(t, c, column, every).astype(jnp.bfloat16)
                pieces = tuple(range(column // size, (column + LANES) // size))
                for q in pieces:
                    state_on[t + 1, q, here] = value[:, q * size - column : (q + 1) * size - column]
                cut = c == CHUNKS - 1 and pieces not in ROUNDS
                send_onward(t + 1, c, [p for p in ROUNDS if p[0] in pieces] if cut else (pieces,))
            for k in sides:
                for column in range(0, lateral, LANES):
                    value = block(t, c, starts[k] + column, every).astype(jnp.bfloat16)
                    state_side[t + 1, k - PIECES, here, column : column + LANES] = value
                to_side(t + 1, c, k).start()

    columns = range(0, width, LANES)
    for c in range(CHUNKS - 1):
        sideways(last, c)
        arrive(last, c, every)
        for column in columns:
            early[rows_of(c), column : column + LANES] = block(last, c, column, every).astype(jnp.bfloat16)
    c = CHUNKS - 1
    here = rows_of(c)
    sideways(last, c)
    for pieces in ROUNDS[:-1]:
        arrive(last, c, pieces)
        for column in columns:
            total[here, column : column + LANES] = block(last, c, column, pieces)
    arrive(last, c, ROUNDS[-1])
    tail[...] = jnp.concatenate([got_on[last, q, here] for q in ROUNDS[-1]], axis=1)

    copy_to(near, state_side, got_side, 1, side_sem.at[0, 0]).wait_send()

    @pl.when(has_next)
    def _():
        copy_to(me + STRIPS, state_on, got_on, 0, on_sem.at[0]).wait_send()


def finish(early, total, mapped, tail, out, late, sem):
    done, width = early.shape
    depth = tail.shape[1]
    bulk = pltpu.make_async_copy(early, out.at[0, pl.ds(0, done)], sem.at[0])
    bulk.start()
    for column in range(0, width, LANES):
        at = pl.ds(column, LANES)
        late[:, at] = (total[done:, at] + dot(tail[...], mapped[mapped.shape[0] - depth :, at])).astype(jnp.bfloat16)
        pltpu.make_async_copy(late.at[:, at], out.at[0, pl.ds(done, late.shape[0]), at], sem.at[1]).start()
    bulk.wait()
    pltpu.make_async_copy(late, out.at[0, pl.ds(done, late.shape[0])], sem.at[1]).wait()


def on_device(count, traces, operator, loads, seeds, patches, trace_map):
    _, rows, width = traces.shape
    onward = trace_map.shape[1]
    lateral = (width - onward) // 2
    depth = loads.shape[1]
    bf16, i32 = jnp.bfloat16, jnp.int32
    anywhere = pl.BlockSpec(memory_space=pltpu.HBM)
    dma = pltpu.SemaphoreType.DMA
    slots = (
        pltpu.VMEM((TICKS, PIECES, rows, onward // PIECES), bf16),
        pltpu.VMEM((TICKS, 2, rows, lateral), bf16),
    )
    local = pl.BlockSpec(memory_space=pltpu.VMEM)
    part = rows // CHUNKS
    parts = pl.pallas_call(
        functools.partial(kernel, count),
        name="sweep",
        out_shape=(
            pltpu.VMEM((rows - part, width), bf16),
            pltpu.VMEM((rows, width), jnp.float32),
            pltpu.VMEM((onward, width), bf16),
            pltpu.VMEM((part, len(ROUNDS[-1]) * (onward // PIECES)), bf16),
        ),
        in_specs=[anywhere] * 6,
        out_specs=(local,) * 4,
        scratch_shapes=[
            pltpu.VMEM((width + depth, width), bf16),
            pltpu.VMEM((onward, onward), bf16),
            *slots,
            *slots,
            pltpu.VMEM((1, onward + 2 * rows), i32),
            pltpu.VMEM((TICKS, depth, rows), bf16),
            dma((3,)),
            dma((2,)),
            dma((TICKS * CHUNKS + len(ROUNDS) - 1,)),
            dma((2, CHUNKS)),
        ],
        compiler_params=pltpu.CompilerParams(
            collective_id=0, has_side_effects=True, vmem_limit_bytes=50 * 2**20
        ),
    )(traces, operator, loads, seeds.reshape(1, rows), patches, trace_map)
    return pl.pallas_call(
        finish,
        name="finish",
        out_shape=jax.ShapeDtypeStruct(traces.shape, bf16),
        in_specs=[local] * 4,
        out_specs=anywhere,
        scratch_shapes=[pltpu.VMEM((part, width), bf16), dma((2,))],
        compiler_params=pltpu.CompilerParams(vmem_limit_bytes=4 * 2**20),
    )(*parts)


def solution(mesh):
    placed = (
        P("bay", "groups", None),
        P("bay", None, None),
        P("bay", None, None),
        P("groups"),
        P("bay", "groups"),
        P("bay", None),
    )
    return jax.shard_map(
        functools.partial(on_device, mesh.shape["bay"]),
        mesh=mesh,
        in_specs=placed,
        out_specs=P("bay", "groups", None),
        check_vma=False,
    )
```

```python
import functools

import jax
import jax.numpy as jnp
from jax import lax
from jax.experimental import pallas as pl
from jax.experimental.pallas import tpu as pltpu
from jax.sharding import PartitionSpec as P

TICKS = 6
STRIPS = 4
CHUNKS = 2
PIECES = 4
ROUNDS = ((0, 1), (2,), (3,))
DEFER = 3
PERIOD = 97
LANES = 512
MESH = pl.DeviceIdType.MESH


def dot(a, b):
    return jnp.dot(a, b, preferred_element_type=jnp.float32)


def kernel(
    count, traces, operator, loads, seeds, patches, trace_map, early, total, mapped, tail,
    weights, one_hot, state_on, state_side, got_on, got_side,
    small, picked,
    send_sem, end_sem,
):
    me = lax.axis_index("bay")
    next_device = {"bay": me + STRIPS}
    has_next = me + STRIPS < count
    has_prev = me >= STRIPS
    part = state_on.shape[2] // CHUNKS
    final = (TICKS - 1, pl.ds(ROUNDS[-1][0], len(ROUNDS[-1])), pl.ds((CHUNKS - 1) * part, part))

    def onward_copy(at, signal):
        return pltpu.make_async_remote_copy(
            src_ref=state_on.at[at],
            dst_ref=got_on.at[at],
            send_sem=send_sem.at[0],
            recv_sem=signal,
            device_id=next_device,
            device_id_type=MESH,
        )

    dma = pltpu.SemaphoreType.DMA
    pl.run_scoped(
        functools.partial(
            sweep, count, traces, operator, loads, seeds, patches, trace_map, early, total, mapped,
            weights, one_hot, state_on, state_side, got_on, got_side, small, picked, send_sem, end_sem,
        ),
        dma((3,)),
        dma((TICKS * CHUNKS + len(ROUNDS) - 2,)),
        dma((2, CHUNKS)),
    )

    @pl.when(has_prev)
    def _():
        onward_copy(final, end_sem.at[0]).wait_recv()

    at, pieces, here = final
    tail[...] = jnp.concatenate([got_on[at, q, here] for q in ROUNDS[-1]], axis=1)
    pltpu.make_async_copy(state_side, state_side, send_sem.at[1]).wait()

    @pl.when(has_next)
    def _():
        pltpu.make_async_copy(state_on, state_on, send_sem.at[0]).wait()


def sweep(
    count, traces, operator, loads, seeds, patches, trace_map, early, total, mapped,
    weights, one_hot, state_on, state_side, got_on, got_side,
    small, picked, send_sem, end_sem,
    in_sem, on_sem, side_sem,
):
    me = lax.axis_index("bay")
    rows, size = state_on.shape[2:]
    lateral = state_side.shape[3]
    onward = PIECES * size
    width = onward + 2 * lateral
    depth = loads.shape[1]
    part = rows // CHUNKS
    has_next = me + STRIPS < count
    has_prev = me >= STRIPS
    near = me + 1 - 2 * (me % 2)
    far = me + 2 - 4 * ((me // 2) % 2)
    barrier = pltpu.get_barrier_semaphore()

    def greet(device):
        pl.semaphore_signal(barrier, inc=1, device_id={"bay": device}, device_id_type=MESH)

    @pl.when(has_prev)
    def _():
        greet(me - STRIPS)

    greet(far)
    greet(near)

    starts = tuple(q * size for q in range(PIECES)) + (onward, onward + lateral)
    sizes = (size,) * PIECES + (lateral, lateral)
    sides = (PIECES, PIECES + 1)

    def rows_of(c):
        return pl.ds(c * part, part)

    def span(pieces):
        return pl.ds(pieces[0], len(pieces))

    def held(t, c, k):
        if k < PIECES:
            return state_on.at[t, k, rows_of(c)]
        return state_side.at[t, k - PIECES, rows_of(c)]

    first = [
        pltpu.make_async_copy(
            traces.at[0, rows_of(c), pl.ds(starts[k], sizes[k])], held(0, c, k), in_sem.at[k // PIECES]
        )
        for c in range(CHUNKS)
        for k in range(PIECES + 2)
    ]
    lists = [
        pltpu.make_async_copy(src, small.at[:, pl.ds(begin, src.shape[1])], in_sem.at[2])
        for src, begin in ((trace_map, 0), (seeds, onward), (patches, onward + rows))
    ]
    upper = pltpu.make_async_copy(operator.at[0, pl.ds(0, onward)], weights.at[pl.ds(0, onward)], in_sem.at[0])
    lower = [
        pltpu.make_async_copy(operator.at[0, pl.ds(onward, onward)], weights.at[pl.ds(onward, onward)], in_sem.at[1]),
        pltpu.make_async_copy(loads.at[0], weights.at[pl.ds(width, depth)], in_sem.at[1]),
    ]
    for copy in first + lists:
        copy.start()

    pl.semaphore_wait(barrier, 2 + has_next.astype(jnp.int32))

    last = TICKS - 1

    def copy_to(device, src, dst, kind, signal):
        return pltpu.make_async_remote_copy(
            src_ref=src,
            dst_ref=dst,
            send_sem=send_sem.at[kind],
            recv_sem=signal,
            device_id={"bay": device},
            device_id_type=MESH,
        )

    def to_next(t, c, pieces):
        signal = on_sem.at[t * CHUNKS + c]
        if isinstance(t, int) and t == last and c == CHUNKS - 1:
            order = ROUNDS.index(pieces)
            signal = end_sem.at[0] if order == len(ROUNDS) - 1 else on_sem.at[t * CHUNKS + c + order]
        here = (t, span(pieces), rows_of(c))
        return copy_to(me + STRIPS, state_on.at[here], got_on.at[here], 0, signal)

    def to_side(t, c, k):
        here = (t, k - PIECES, rows_of(c))
        return copy_to((near, far)[k - PIECES], state_side.at[here], got_side.at[here], 1, side_sem.at[t % 2, c])

    def both_sides(t, c):
        here = (t, slice(None), rows_of(c))
        return copy_to(near, state_side.at[here], got_side.at[here], 1, side_sem.at[t % 2, c])

    def send_onward(t, c, groups):
        @pl.when(has_next)
        def _():
            for pieces in groups:
                to_next(t, c, pieces).start()

    def loaded(ref, which):
        pltpu.make_async_copy(ref, ref, in_sem.at[which]).wait()

    every = tuple(range(PIECES))
    deferred = jnp.logical_not(has_prev) & (me % 2 == 1)

    def send_first(c, when):
        @pl.when(has_next & when)
        def _():
            to_next(0, c, every).start()

    loaded(state_on.at[0], 0)
    send_first(0, True)
    for c in range(1, CHUNKS):
        send_first(c, jnp.logical_not(deferred))
    loaded(state_side.at[0], 1)
    for c in range(CHUNKS):
        for k in sides:
            to_side(0, c, k).start()
    for copy in [upper] + lower:
        copy.start()

    @pl.when(jnp.logical_not(has_prev))
    def _():
        got_on[...] = jnp.zeros_like(got_on)

    loaded(small, 2)
    map_row = small[:, :onward]
    seed_row = small[:, onward : onward + rows]
    pick_row = small[:, onward + rows :]
    place = lax.broadcasted_iota(jnp.int32, one_hot.shape, 0)
    one_hot[...] = jnp.where(place == map_row, 1.0, 0.0).astype(jnp.bfloat16)
    value = seed_row * 7
    guess = (value.astype(jnp.float32) * (1.0 / PERIOD)).astype(jnp.int32)
    rest = value - guess * PERIOD
    rest = jnp.where(rest < 0, rest + PERIOD, rest)
    rest = jnp.where(rest >= PERIOD, rest - PERIOD, rest)
    chosen = lax.broadcasted_iota(jnp.int32, picked.shape[1:], 0) == pick_row
    for t in range(TICKS):
        turn = rest + (13 * t) % PERIOD
        turn = jnp.where(turn >= PERIOD, turn - PERIOD, turn)
        amplitude = (turn - 48).astype(jnp.float32) / 32.0
        picked[t] = jnp.where(chosen, amplitude, 0.0).astype(jnp.bfloat16)

    upper.wait()

    @pl.loop(0, width // LANES)
    def _(n):
        at = pl.ds(pl.multiple_of(n * LANES, LANES), LANES)
        for m in range(0, onward, 256):
            mapped[m : m + 256, at] = dot(one_hot[m : m + 256, :], weights[:onward, at]).astype(jnp.bfloat16)

        for c in range(1, CHUNKS):
            send_first(c, deferred & (n == DEFER))

    loaded(weights.at[pl.ds(onward, onward + depth)], 1)

    def sideways(t, c):
        here = rows_of(c)
        both_sides(t, c).wait_recv()

        @pl.loop(0, width // LANES)
        def _(n):
            at = pl.ds(pl.multiple_of(n * LANES, LANES), LANES)
            source = lax.dot_general(
                picked[t, :, here], weights[width:, at], (((0,), (0,)), ((), ())), preferred_element_type=jnp.float32
            )
            total[here, at] = (
                source
                + dot(got_side[t, 0, here], weights[onward : onward + lateral, at])
                + dot(got_side[t, 1, here], weights[onward + lateral : width, at])
            )

    def arrive(t, c, pieces):
        @pl.when(has_prev)
        def _():
            to_next(t, c, pieces).wait_recv()

    def block(t, c, column, pieces):
        here = rows_of(c)
        at = pl.ds(column, LANES)
        incoming = jnp.concatenate([got_on[t, q, here] for q in pieces], axis=1)
        return total[here, at] + dot(incoming, mapped[pieces[0] * size : (pieces[-1] + 1) * size, at])

    def tick(t):
        for c in range(CHUNKS):
            here = rows_of(c)
            sideways(t, c)
            arrive(t, c, every)
            for column in range(0, onward, LANES):
                value = block(t, c, column, every).astype(jnp.bfloat16)
                pieces = tuple(range(column // size, (column + LANES) // size))
                for q in pieces:
                    state_on[t + 1, q, here] = value[:, q * size - column : (q + 1) * size - column]
                cut = isinstance(t, int) and c == CHUNKS - 1
                send_onward(t + 1, c, [p for p in ROUNDS if p[0] in pieces] if cut else (pieces,))
            for k in sides:
                for column in range(0, lateral, LANES):
                    value = block(t, c, starts[k] + column, every).astype(jnp.bfloat16)
                    state_side[t + 1, k - PIECES, here, column : column + LANES] = value
                to_side(t + 1, c, k).start()

    pl.loop(0, TICKS - 2)(tick)
    tick(TICKS - 2)

    columns = range(0, width, LANES)
    for c in range(CHUNKS - 1):
        sideways(last, c)
        arrive(last, c, every)
        for column in columns:
            early[rows_of(c), column : column + LANES] = block(last, c, column, every).astype(jnp.bfloat16)
    c = CHUNKS - 1
    here = rows_of(c)
    sideways(last, c)
    for pieces in ROUNDS[:-1]:
        arrive(last, c, pieces)
        for column in columns:
            total[here, column : column + LANES] = block(last, c, column, pieces)


def finish(early, total, mapped, tail, out, late, sem):
    done, width = early.shape
    depth = tail.shape[1]
    bulk = pltpu.make_async_copy(early, out.at[0, pl.ds(0, done)], sem.at[0])
    bulk.start()
    for column in range(0, width, LANES):
        at = pl.ds(column, LANES)
        late[:, at] = (total[done:, at] + dot(tail[...], mapped[mapped.shape[0] - depth :, at])).astype(jnp.bfloat16)
        pltpu.make_async_copy(late.at[:, at], out.at[0, pl.ds(done, late.shape[0]), at], sem.at[1]).start()
    bulk.wait()
    pltpu.make_async_copy(late, out.at[0, pl.ds(done, late.shape[0])], sem.at[1]).wait()


def on_device(count, traces, operator, loads, seeds, patches, trace_map):
    _, rows, width = traces.shape
    onward = trace_map.shape[1]
    lateral = (width - onward) // 2
    depth = loads.shape[1]
    bf16, i32 = jnp.bfloat16, jnp.int32
    anywhere = pl.BlockSpec(memory_space=pltpu.HBM)
    dma = pltpu.SemaphoreType.DMA
    slots = (
        pltpu.VMEM((TICKS, PIECES, rows, onward // PIECES), bf16),
        pltpu.VMEM((TICKS, 2, rows, lateral), bf16),
    )
    local = pl.BlockSpec(memory_space=pltpu.VMEM)
    part = rows // CHUNKS
    parts = pl.pallas_call(
        functools.partial(kernel, count),
        name="sweep",
        out_shape=(
            pltpu.VMEM((rows - part, width), bf16),
            pltpu.VMEM((rows, width), jnp.float32),
            pltpu.VMEM((onward, width), bf16),
            pltpu.VMEM((part, len(ROUNDS[-1]) * (onward // PIECES)), bf16),
        ),
        in_specs=[anywhere] * 6,
        out_specs=(local,) * 4,
        scratch_shapes=[
            pltpu.VMEM((width + depth, width), bf16),
            pltpu.VMEM((onward, onward), bf16),
            *slots,
            *slots,
            pltpu.VMEM((1, onward + 2 * rows), i32),
            pltpu.VMEM((TICKS, depth, rows), bf16),
            dma((2,)),
            dma((1,)),
        ],
        compiler_params=pltpu.CompilerParams(
            collective_id=0, has_side_effects=True, vmem_limit_bytes=50 * 2**20
        ),
    )(traces, operator, loads, seeds.reshape(1, rows), patches, trace_map)
    return pl.pallas_call(
        finish,
        name="finish",
        out_shape=jax.ShapeDtypeStruct(traces.shape, bf16),
        in_specs=[local] * 4,
        out_specs=anywhere,
        scratch_shapes=[pltpu.VMEM((part, width), bf16), dma((2,))],
        compiler_params=pltpu.CompilerParams(vmem_limit_bytes=4 * 2**20),
    )(*parts)


def solution(mesh):
    placed = (
        P("bay", "groups", None),
        P("bay", None, None),
        P("bay", None, None),
        P("groups"),
        P("bay", "groups"),
        P("bay", None),
    )
    return jax.shard_map(
        functools.partial(on_device, mesh.shape["bay"]),
        mesh=mesh,
        in_specs=placed,
        out_specs=P("bay", "groups", None),
        check_vma=False,
    )
```

```python
import functools

import jax
import jax.numpy as jnp
from jax import lax
from jax.experimental import pallas as pl
from jax.experimental.pallas import tpu as pltpu
from jax.sharding import PartitionSpec as P

TICKS = 6
STRIPS = 4
CHUNKS = 2
PIECES = 4
ROUNDS = ((0, 1), (2,), (3,))
DEFER = 3
PERIOD = 97
LANES = 512
MESH = pl.DeviceIdType.MESH


def dot(a, b):
    return jnp.dot(a, b, preferred_element_type=jnp.float32)


def kernel(
    count, traces, operator, loads, seeds, patches, trace_map, early, total, mapped, tail,
    weights, one_hot, state_on, state_side, got_on, got_side,
    small, picked,
    send_sem, end_sem,
):
    me = lax.axis_index("bay")
    next_device = {"bay": me + STRIPS}
    has_next = me + STRIPS < count
    has_prev = me >= STRIPS
    part = state_on.shape[2] // CHUNKS
    final = (TICKS - 1, pl.ds(ROUNDS[-1][0], len(ROUNDS[-1])), pl.ds((CHUNKS - 1) * part, part))

    def onward_copy(at, signal):
        return pltpu.make_async_remote_copy(
            src_ref=state_on.at[at],
            dst_ref=got_on.at[at],
            send_sem=send_sem,
            recv_sem=signal,
            device_id=next_device,
            device_id_type=MESH,
        )

    dma = pltpu.SemaphoreType.DMA
    pl.run_scoped(
        functools.partial(
            sweep, count, traces, operator, loads, seeds, patches, trace_map, early, total, mapped,
            weights, one_hot, state_on, state_side, got_on, got_side, small, picked, send_sem, end_sem,
        ),
        dma((3,)),
        dma((TICKS * CHUNKS + len(ROUNDS) - 2,)),
        dma((2, CHUNKS)),
        dma(()),
    )

    @pl.when(has_prev)
    def _():
        onward_copy(final, end_sem).wait_recv()

    at, pieces, here = final
    tail[...] = jnp.concatenate([got_on[at, q, here] for q in ROUNDS[-1]], axis=1)

    @pl.when(has_next)
    def _():
        pltpu.make_async_copy(state_on, state_on, send_sem).wait()


def sweep(
    count, traces, operator, loads, seeds, patches, trace_map, early, total, mapped,
    weights, one_hot, state_on, state_side, got_on, got_side,
    small, picked, send_sem, end_sem,
    in_sem, on_sem, side_sem, side_send,
):
    me = lax.axis_index("bay")
    rows, size = state_on.shape[2:]
    lateral = state_side.shape[3]
    onward = PIECES * size
    width = onward + 2 * lateral
    depth = loads.shape[1]
    part = rows // CHUNKS
    has_next = me + STRIPS < count
    has_prev = me >= STRIPS
    near = me + 1 - 2 * (me % 2)
    far = me + 2 - 4 * ((me // 2) % 2)
    barrier = pltpu.get_barrier_semaphore()

    def greet(device):
        pl.semaphore_signal(barrier, inc=1, device_id={"bay": device}, device_id_type=MESH)

    @pl.when(has_prev)
    def _():
        greet(me - STRIPS)

    greet(far)
    greet(near)

    starts = tuple(q * size for q in range(PIECES)) + (onward, onward + lateral)
    sizes = (size,) * PIECES + (lateral, lateral)
    sides = (PIECES, PIECES + 1)

    def rows_of(c):
        return pl.ds(c * part, part)

    def span(pieces):
        return pl.ds(pieces[0], len(pieces))

    def held(t, c, k):
        if k < PIECES:
            return state_on.at[t, k, rows_of(c)]
        return state_side.at[t, k - PIECES, rows_of(c)]

    first = [
        pltpu.make_async_copy(
            traces.at[0, rows_of(c), pl.ds(starts[k], sizes[k])], held(0, c, k), in_sem.at[k // PIECES]
        )
        for c in range(CHUNKS)
        for k in range(PIECES + 2)
    ]
    lists = [
        pltpu.make_async_copy(src, small.at[:, pl.ds(begin, src.shape[1])], in_sem.at[2])
        for src, begin in ((trace_map, 0), (seeds, onward), (patches, onward + rows))
    ]
    upper = pltpu.make_async_copy(operator.at[0, pl.ds(0, onward)], weights.at[pl.ds(0, onward)], in_sem.at[0])
    lower = [
        pltpu.make_async_copy(operator.at[0, pl.ds(onward, onward)], weights.at[pl.ds(onward, onward)], in_sem.at[1]),
        pltpu.make_async_copy(loads.at[0], weights.at[pl.ds(width, depth)], in_sem.at[1]),
    ]
    for copy in first + lists:
        copy.start()

    pl.semaphore_wait(barrier, 2 + has_next.astype(jnp.int32))

    last = TICKS - 1

    def copy_to(device, src, dst, kind, signal):
        return pltpu.make_async_remote_copy(
            src_ref=src,
            dst_ref=dst,
            send_sem=(send_sem, side_send)[kind],
            recv_sem=signal,
            device_id={"bay": device},
            device_id_type=MESH,
        )

    def to_next(t, c, pieces):
        signal = on_sem.at[t * CHUNKS + c]
        if isinstance(t, int) and t == last and c == CHUNKS - 1:
            order = ROUNDS.index(pieces)
            signal = end_sem if order == len(ROUNDS) - 1 else on_sem.at[t * CHUNKS + c + order]
        here = (t, span(pieces), rows_of(c))
        return copy_to(me + STRIPS, state_on.at[here], got_on.at[here], 0, signal)

    def to_side(t, c, k):
        here = (t, k - PIECES, rows_of(c))
        return copy_to((near, far)[k - PIECES], state_side.at[here], got_side.at[here], 1, side_sem.at[t % 2, c])

    def both_sides(t, c):
        here = (t, slice(None), rows_of(c))
        return copy_to(near, state_side.at[here], got_side.at[here], 1, side_sem.at[t % 2, c])

    def send_onward(t, c, groups):
        @pl.when(has_next)
        def _():
            for pieces in groups:
                to_next(t, c, pieces).start()

    def loaded(ref, which):
        pltpu.make_async_copy(ref, ref, in_sem.at[which]).wait()

    every = tuple(range(PIECES))
    deferred = jnp.logical_not(has_prev) & (me % 2 == 1)

    def send_first(c, when):
        @pl.when(has_next & when)
        def _():
            to_next(0, c, every).start()

    loaded(state_on.at[0], 0)
    send_first(0, True)
    for c in range(1, CHUNKS):
        send_first(c, jnp.logical_not(deferred))
    loaded(state_side.at[0], 1)
    for c in range(CHUNKS):
        for k in sides:
            to_side(0, c, k).start()
    for copy in [upper] + lower:
        copy.start()

    @pl.when(jnp.logical_not(has_prev))
    def _():
        got_on[...] = jnp.zeros_like(got_on)

    loaded(small, 2)
    map_row = small[:, :onward]
    seed_row = small[:, onward : onward + rows]
    pick_row = small[:, onward + rows :]
    place = lax.broadcasted_iota(jnp.int32, one_hot.shape, 0)
    one_hot[...] = jnp.where(place == map_row, 1.0, 0.0).astype(jnp.bfloat16)
    value = seed_row * 7
    guess = (value.astype(jnp.float32) * (1.0 / PERIOD)).astype(jnp.int32)
    rest = value - guess * PERIOD
    rest = jnp.where(rest < 0, rest + PERIOD, rest)
    rest = jnp.where(rest >= PERIOD, rest - PERIOD, rest)
    chosen = lax.broadcasted_iota(jnp.int32, picked.shape[1:], 0) == pick_row
    for t in range(TICKS):
        turn = rest + (13 * t) % PERIOD
        turn = jnp.where(turn >= PERIOD, turn - PERIOD, turn)
        amplitude = (turn - 48).astype(jnp.float32) / 32.0
        picked[t] = jnp.where(chosen, amplitude, 0.0).astype(jnp.bfloat16)

    upper.wait()

    @pl.loop(0, width // LANES)
    def _(n):
        at = pl.ds(pl.multiple_of(n * LANES, LANES), LANES)
        for m in range(0, onward, 256):
            mapped[m : m + 256, at] = dot(one_hot[m : m + 256, :], weights[:onward, at]).astype(jnp.bfloat16)

        for c in range(1, CHUNKS):
            send_first(c, deferred & (n == DEFER))

    loaded(weights.at[pl.ds(onward, onward + depth)], 1)

    def sideways(t, c):
        here = rows_of(c)
        both_sides(t, c).wait_recv()

        @pl.loop(0, width // LANES)
        def _(n):
            at = pl.ds(pl.multiple_of(n * LANES, LANES), LANES)
            source = lax.dot_general(
                picked[t, :, here], weights[width:, at], (((0,), (0,)), ((), ())), preferred_element_type=jnp.float32
            )
            total[here, at] = (
                source
                + dot(got_side[t, 0, here], weights[onward : onward + lateral, at])
                + dot(got_side[t, 1, here], weights[onward + lateral : width, at])
            )

    def arrive(t, c, pieces):
        @pl.when(has_prev)
        def _():
            to_next(t, c, pieces).wait_recv()

    def block(t, c, column, pieces):
        here = rows_of(c)
        at = pl.ds(column, LANES)
        incoming = jnp.concatenate([got_on[t, q, here] for q in pieces], axis=1)
        return total[here, at] + dot(incoming, mapped[pieces[0] * size : (pieces[-1] + 1) * size, at])

    def tick(t):
        for c in range(CHUNKS):
            here = rows_of(c)
            sideways(t, c)
            arrive(t, c, every)
            for column in range(0, onward, LANES):
                value = block(t, c, column, every).astype(jnp.bfloat16)
                pieces = tuple(range(column // size, (column + LANES) // size))
                for q in pieces:
                    state_on[t + 1, q, here] = value[:, q * size - column : (q + 1) * size - column]
                cut = isinstance(t, int) and c == CHUNKS - 1
                send_onward(t + 1, c, [p for p in ROUNDS if p[0] in pieces] if cut else (pieces,))
            for k in sides:
                for column in range(0, lateral, LANES):
                    value = block(t, c, starts[k] + column, every).astype(jnp.bfloat16)
                    state_side[t + 1, k - PIECES, here, column : column + LANES] = value
                to_side(t + 1, c, k).start()

    pl.loop(0, TICKS - 2)(tick)
    tick(TICKS - 2)

    columns = range(0, width, LANES)
    for c in range(CHUNKS - 1):
        sideways(last, c)
        arrive(last, c, every)
        for column in columns:
            early[rows_of(c), column : column + LANES] = block(last, c, column, every).astype(jnp.bfloat16)
    c = CHUNKS - 1
    here = rows_of(c)
    sideways(last, c)
    for pieces in ROUNDS[:-1]:
        arrive(last, c, pieces)
        for column in columns:
            total[here, column : column + LANES] = block(last, c, column, pieces)
    pltpu.make_async_copy(state_side, state_side, side_send).wait()


def finish(early, total, mapped, tail, out, late, sem):
    done, width = early.shape
    depth = tail.shape[1]
    bulk = pltpu.make_async_copy(early, out.at[0, pl.ds(0, done)], sem.at[0])
    bulk.start()
    for column in range(0, width, LANES):
        at = pl.ds(column, LANES)
        late[:, at] = (total[done:, at] + dot(tail[...], mapped[mapped.shape[0] - depth :, at])).astype(jnp.bfloat16)
        pltpu.make_async_copy(late.at[:, at], out.at[0, pl.ds(done, late.shape[0]), at], sem.at[1]).start()
    bulk.wait()
    pltpu.make_async_copy(late, out.at[0, pl.ds(done, late.shape[0])], sem.at[1]).wait()


def on_device(count, traces, operator, loads, seeds, patches, trace_map):
    _, rows, width = traces.shape
    onward = trace_map.shape[1]
    lateral = (width - onward) // 2
    depth = loads.shape[1]
    bf16, i32 = jnp.bfloat16, jnp.int32
    anywhere = pl.BlockSpec(memory_space=pltpu.HBM)
    dma = pltpu.SemaphoreType.DMA
    slots = (
        pltpu.VMEM((TICKS, PIECES, rows, onward // PIECES), bf16),
        pltpu.VMEM((TICKS, 2, rows, lateral), bf16),
    )
    local = pl.BlockSpec(memory_space=pltpu.VMEM)
    part = rows // CHUNKS
    parts = pl.pallas_call(
        functools.partial(kernel, count),
        name="sweep",
        out_shape=(
            pltpu.VMEM((rows - part, width), bf16),
            pltpu.VMEM((rows, width), jnp.float32),
            pltpu.VMEM((onward, width), bf16),
            pltpu.VMEM((part, len(ROUNDS[-1]) * (onward // PIECES)), bf16),
        ),
        in_specs=[anywhere] * 6,
        out_specs=(local,) * 4,
        scratch_shapes=[
            pltpu.VMEM((width + depth, width), bf16),
            pltpu.VMEM((onward, onward), bf16),
            *slots,
            *slots,
            pltpu.VMEM((1, onward + 2 * rows), i32),
            pltpu.VMEM((TICKS, depth, rows), bf16),
            dma(()),
            dma(()),
        ],
        compiler_params=pltpu.CompilerParams(
            collective_id=0, has_side_effects=True, vmem_limit_bytes=50 * 2**20
        ),
    )(traces, operator, loads, seeds.reshape(1, rows), patches, trace_map)
    return pl.pallas_call(
        finish,
        name="finish",
        out_shape=jax.ShapeDtypeStruct(traces.shape, bf16),
        in_specs=[local] * 4,
        out_specs=anywhere,
        scratch_shapes=[pltpu.VMEM((part, width), bf16), dma((2,))],
        compiler_params=pltpu.CompilerParams(vmem_limit_bytes=4 * 2**20),
    )(*parts)


def solution(mesh):
    placed = (
        P("bay", "groups", None),
        P("bay", None, None),
        P("bay", None, None),
        P("groups"),
        P("bay", "groups"),
        P("bay", None),
    )
    return jax.shard_map(
        functools.partial(on_device, mesh.shape["bay"]),
        mesh=mesh,
        in_specs=placed,
        out_specs=P("bay", "groups", None),
        check_vma=False,
    )
```

```python
import functools

import jax
import jax.numpy as jnp
from jax import lax
from jax.experimental import pallas as pl
from jax.experimental.pallas import tpu as pltpu
from jax.sharding import PartitionSpec as P

TICKS = 6
STRIPS = 4
CHUNKS = 2
PIECES = 4
ROUNDS = ((0, 1), (2,), (3,))
DEFER = 3
PERIOD = 97
LANES = 512
MESH = pl.DeviceIdType.MESH


def dot(a, b):
    return jnp.dot(a, b, preferred_element_type=jnp.float32)


def kernel(
    count, traces, operator, loads, seeds, patches, trace_map, early, total, mapped, tail,
    weights, one_hot, state_on, state_side, got_on, got_side,
    small, picked,
    send_sem, end_sem,
):
    me = lax.axis_index("bay")
    next_device = {"bay": me + STRIPS}
    has_next = me + STRIPS < count
    has_prev = me >= STRIPS
    part = state_on.shape[2] // CHUNKS
    final = (TICKS - 1, pl.ds(ROUNDS[-1][0], len(ROUNDS[-1])), pl.ds((CHUNKS - 1) * part, part))

    def onward_copy(at, signal):
        return pltpu.make_async_remote_copy(
            src_ref=state_on.at[at],
            dst_ref=got_on.at[at],
            send_sem=send_sem,
            recv_sem=signal,
            device_id=next_device,
            device_id_type=MESH,
        )

    dma = pltpu.SemaphoreType.DMA
    pl.run_scoped(
        functools.partial(
            sweep, count, traces, operator, loads, seeds, patches, trace_map, early, total, mapped,
            weights, one_hot, state_on, state_side, got_on, got_side, small, picked, send_sem, end_sem,
        ),
        dma((3,)),
        dma((TICKS * CHUNKS + len(ROUNDS) - 2,)),
        dma((2, CHUNKS)),
        dma(()),
    )

    @pl.when(has_prev)
    def _():
        onward_copy(final, end_sem).wait_recv()

    at, pieces, here = final
    tail[...] = jnp.concatenate([got_on[at, q, here] for q in ROUNDS[-1]], axis=1)

    @pl.when(has_next)
    def _():
        pltpu.make_async_copy(state_on, state_on, send_sem).wait()


def sweep(
    count, traces, operator, loads, seeds, patches, trace_map, early, total, mapped,
    weights, one_hot, state_on, state_side, got_on, got_side,
    small, picked, send_sem, end_sem,
    in_sem, on_sem, side_sem, side_send,
):
    me = lax.axis_index("bay")
    rows, size = state_on.shape[2:]
    lateral = state_side.shape[3]
    onward = PIECES * size
    width = onward + 2 * lateral
    depth = loads.shape[1]
    part = rows // CHUNKS
    has_next = me + STRIPS < count
    has_prev = me >= STRIPS
    near = me + 1 - 2 * (me % 2)
    far = me + 2 - 4 * ((me // 2) % 2)
    barrier = pltpu.get_barrier_semaphore()

    def greet(device):
        pl.semaphore_signal(barrier, inc=1, device_id={"bay": device}, device_id_type=MESH)

    @pl.when(has_prev)
    def _():
        greet(me - STRIPS)

    greet(far)
    greet(near)

    starts = tuple(q * size for q in range(PIECES)) + (onward, onward + lateral)
    sizes = (size,) * PIECES + (lateral, lateral)
    sides = (PIECES, PIECES + 1)

    def rows_of(c):
        return pl.ds(c * part, part)

    def span(pieces):
        return pl.ds(pieces[0], len(pieces))

    def held(t, c, k):
        if k < PIECES:
            return state_on.at[t, k, rows_of(c)]
        return state_side.at[t, k - PIECES, rows_of(c)]

    first = [
        pltpu.make_async_copy(
            traces.at[0, rows_of(c), pl.ds(starts[k], sizes[k])], held(0, c, k), in_sem.at[k // PIECES]
        )
        for c in range(CHUNKS)
        for k in range(PIECES + 2)
    ]
    lists = [
        pltpu.make_async_copy(src, small.at[:, pl.ds(begin, src.shape[1])], in_sem.at[2])
        for src, begin in ((trace_map, 0), (seeds, onward), (patches, onward + rows))
    ]
    upper = pltpu.make_async_copy(operator.at[0, pl.ds(0, onward)], weights.at[pl.ds(0, onward)], in_sem.at[0])
    lower = [
        pltpu.make_async_copy(operator.at[0, pl.ds(onward, onward)], weights.at[pl.ds(onward, onward)], in_sem.at[1]),
        pltpu.make_async_copy(loads.at[0], weights.at[pl.ds(width, depth)], in_sem.at[1]),
    ]
    for copy in first + lists:
        copy.start()

    pl.semaphore_wait(barrier, 2 + has_next.astype(jnp.int32))

    last = TICKS - 1

    def copy_to(device, src, dst, kind, signal):
        return pltpu.make_async_remote_copy(
            src_ref=src,
            dst_ref=dst,
            send_sem=(send_sem, side_send)[kind],
            recv_sem=signal,
            device_id={"bay": device},
            device_id_type=MESH,
        )

    def to_next(t, c, pieces):
        signal = on_sem.at[t * CHUNKS + c]
        if isinstance(t, int) and t == last and c == CHUNKS - 1:
            order = ROUNDS.index(pieces)
            signal = end_sem if order == len(ROUNDS) - 1 else on_sem.at[t * CHUNKS + c + order]
        here = (t, span(pieces), rows_of(c))
        return copy_to(me + STRIPS, state_on.at[here], got_on.at[here], 0, signal)

    def to_side(t, c, k):
        here = (t, k - PIECES, rows_of(c))
        return copy_to((near, far)[k - PIECES], state_side.at[here], got_side.at[here], 1, side_sem.at[t % 2, c])

    def both_sides(t, c):
        here = (t, slice(None), rows_of(c))
        return copy_to(near, state_side.at[here], got_side.at[here], 1, side_sem.at[t % 2, c])

    def send_onward(t, c, groups):
        @pl.when(has_next)
        def _():
            for pieces in groups:
                to_next(t, c, pieces).start()

    def loaded(ref, which):
        pltpu.make_async_copy(ref, ref, in_sem.at[which]).wait()

    every = tuple(range(PIECES))
    deferred = jnp.logical_not(has_prev) & (me % 2 == 1)

    def send_first(c, when):
        @pl.when(has_next & when)
        def _():
            to_next(0, c, every).start()

    loaded(state_on.at[0], 0)
    send_first(0, True)
    for c in range(1, CHUNKS):
        send_first(c, jnp.logical_not(deferred))
    loaded(state_side.at[0], 1)
    for c in range(CHUNKS):
        for k in sides:
            to_side(0, c, k).start()
    @pl.when(jnp.logical_not(has_prev))
    def _():
        got_on[...] = jnp.zeros_like(got_on)

    loaded(small, 2)
    map_row = small[:, :onward]
    seed_row = small[:, onward : onward + rows]
    pick_row = small[:, onward + rows :]
    place = lax.broadcasted_iota(jnp.int32, one_hot.shape, 0)
    one_hot[...] = jnp.where(place == map_row, 1.0, 0.0).astype(jnp.bfloat16)
    value = seed_row * 7
    guess = (value.astype(jnp.float32) * (1.0 / PERIOD)).astype(jnp.int32)
    rest = value - guess * PERIOD
    rest = jnp.where(rest < 0, rest + PERIOD, rest)
    rest = jnp.where(rest >= PERIOD, rest - PERIOD, rest)
    chosen = lax.broadcasted_iota(jnp.int32, picked.shape[1:], 0) == pick_row
    for t in range(TICKS):
        turn = rest + (13 * t) % PERIOD
        turn = jnp.where(turn >= PERIOD, turn - PERIOD, turn)
        amplitude = (turn - 48).astype(jnp.float32) / 32.0
        picked[t] = jnp.where(chosen, amplitude, 0.0).astype(jnp.bfloat16)

    upper.start()
    upper.wait()
    for copy in lower:
        copy.start()

    @pl.loop(0, width // LANES)
    def _(n):
        at = pl.ds(pl.multiple_of(n * LANES, LANES), LANES)
        for m in range(0, onward, 256):
            mapped[m : m + 256, at] = dot(one_hot[m : m + 256, :], weights[:onward, at]).astype(jnp.bfloat16)

        for c in range(1, CHUNKS):
            send_first(c, deferred & (n == DEFER))

    loaded(weights.at[pl.ds(onward, onward + depth)], 1)

    def sideways(t, c):
        here = rows_of(c)
        both_sides(t, c).wait_recv()

        @pl.loop(0, width // LANES)
        def _(n):
            at = pl.ds(pl.multiple_of(n * LANES, LANES), LANES)
            source = lax.dot_general(
                picked[t, :, here], weights[width:, at], (((0,), (0,)), ((), ())), preferred_element_type=jnp.float32
            )
            total[here, at] = (
                source
                + dot(got_side[t, 0, here], weights[onward : onward + lateral, at])
                + dot(got_side[t, 1, here], weights[onward + lateral : width, at])
            )

    def arrive(t, c, pieces):
        @pl.when(has_prev)
        def _():
            to_next(t, c, pieces).wait_recv()

    def block(t, c, column, pieces):
        here = rows_of(c)
        at = pl.ds(column, LANES)
        incoming = jnp.concatenate([got_on[t, q, here] for q in pieces], axis=1)
        return total[here, at] + dot(incoming, mapped[pieces[0] * size : (pieces[-1] + 1) * size, at])

    def tick(t):
        for c in range(CHUNKS):
            here = rows_of(c)
            sideways(t, c)
            arrive(t, c, every)
            for column in range(0, onward, LANES):
                value = block(t, c, column, every).astype(jnp.bfloat16)
                pieces = tuple(range(column // size, (column + LANES) // size))
                for q in pieces:
                    state_on[t + 1, q, here] = value[:, q * size - column : (q + 1) * size - column]
                if isinstance(t, int) and c == CHUNKS - 1:
                    send_onward(t + 1, c, [p for p in ROUNDS if p[0] in pieces])
                elif pieces[-1] == PIECES - 1:
                    send_onward(t + 1, c, (every,))
            for k in sides:
                for column in range(0, lateral, LANES):
                    value = block(t, c, starts[k] + column, every).astype(jnp.bfloat16)
                    state_side[t + 1, k - PIECES, here, column : column + LANES] = value
                to_side(t + 1, c, k).start()

    pl.loop(0, TICKS - 2)(tick)
    tick(TICKS - 2)

    columns = range(0, width, LANES)
    for c in range(CHUNKS - 1):
        sideways(last, c)
        arrive(last, c, every)
        for column in columns:
            early[rows_of(c), column : column + LANES] = block(last, c, column, every).astype(jnp.bfloat16)
    c = CHUNKS - 1
    here = rows_of(c)
    sideways(last, c)
    for pieces in ROUNDS[:-1]:
        arrive(last, c, pieces)
        for column in columns:
            total[here, column : column + LANES] = block(last, c, column, pieces)
    pltpu.make_async_copy(state_side, state_side, side_send).wait()


def finish(early, total, mapped, tail, out, late, sem):
    done, width = early.shape
    depth = tail.shape[1]
    bulk = pltpu.make_async_copy(early, out.at[0, pl.ds(0, done)], sem.at[0])
    bulk.start()
    for column in range(0, width, LANES):
        at = pl.ds(column, LANES)
        late[:, at] = (total[done:, at] + dot(tail[...], mapped[mapped.shape[0] - depth :, at])).astype(jnp.bfloat16)
        pltpu.make_async_copy(late.at[:, at], out.at[0, pl.ds(done, late.shape[0]), at], sem.at[1]).start()
    bulk.wait()
    pltpu.make_async_copy(late, out.at[0, pl.ds(done, late.shape[0])], sem.at[1]).wait()


def on_device(count, traces, operator, loads, seeds, patches, trace_map):
    _, rows, width = traces.shape
    onward = trace_map.shape[1]
    lateral = (width - onward) // 2
    depth = loads.shape[1]
    bf16, i32 = jnp.bfloat16, jnp.int32
    anywhere = pl.BlockSpec(memory_space=pltpu.HBM)
    dma = pltpu.SemaphoreType.DMA
    slots = (
        pltpu.VMEM((TICKS, PIECES, rows, onward // PIECES), bf16),
        pltpu.VMEM((TICKS, 2, rows, lateral), bf16),
    )
    local = pl.BlockSpec(memory_space=pltpu.VMEM)
    part = rows // CHUNKS
    parts = pl.pallas_call(
        functools.partial(kernel, count),
        name="sweep",
        out_shape=(
            pltpu.VMEM((rows - part, width), bf16),
            pltpu.VMEM((rows, width), jnp.float32),
            pltpu.VMEM((onward, width), bf16),
            pltpu.VMEM((part, len(ROUNDS[-1]) * (onward // PIECES)), bf16),
        ),
        in_specs=[anywhere] * 6,
        out_specs=(local,) * 4,
        scratch_shapes=[
            pltpu.VMEM((width + depth, width), bf16),
            pltpu.VMEM((onward, onward), bf16),
            *slots,
            *slots,
            pltpu.VMEM((1, onward + 2 * rows), i32),
            pltpu.VMEM((TICKS, depth, rows), bf16),
            dma(()),
            dma(()),
        ],
        compiler_params=pltpu.CompilerParams(
            collective_id=0, has_side_effects=True, vmem_limit_bytes=50 * 2**20
        ),
    )(traces, operator, loads, seeds.reshape(1, rows), patches, trace_map)
    return pl.pallas_call(
        finish,
        name="finish",
        out_shape=jax.ShapeDtypeStruct(traces.shape, bf16),
        in_specs=[local] * 4,
        out_specs=anywhere,
        scratch_shapes=[pltpu.VMEM((part, width), bf16), dma((2,))],
        compiler_params=pltpu.CompilerParams(vmem_limit_bytes=4 * 2**20),
    )(*parts)


def solution(mesh):
    placed = (
        P("bay", "groups", None),
        P("bay", None, None),
        P("bay", None, None),
        P("groups"),
        P("bay", "groups"),
        P("bay", None),
    )
    return jax.shard_map(
        functools.partial(on_device, mesh.shape["bay"]),
        mesh=mesh,
        in_specs=placed,
        out_specs=P("bay", "groups", None),
        check_vma=False,
    )
```
